64 devices in a mesh: rep: 8 (over x, y, core), dp: 8 (over z).
Axes of the slice: x: 2, y: 2, z: 8, core: 2. Of those that a mesh axis runs over, the one named last changes fastest.
The devices are a block of a 4x4x8 slice.
Arguments:
- x: bfloat16 [64, 4096, 512], P(('rep', 'dp')), parts along dimension 0
- dy: bfloat16 [64, 4096, 512], P(('rep', 'dp')), parts along dimension 0
- w_gate: bfloat16 [2, 512, 2048], replicated
- w_up: bfloat16 [2, 512, 2048], replicated
- w_down: bfloat16 [2, 2048, 512], replicated
- m_w_gate: float32 [2, 512, 2048], replicated
- m_w_up: float32 [2, 512, 2048], replicated
- m_w_down: float32 [2, 2048, 512], replicated
- v_w_gate: float32 [2, 512, 2048], replicated
- v_w_up: float32 [2, 512, 2048], replicated
- v_w_down: float32 [2, 2048, 512], replicated
Outputs:
- output 1: bfloat16 [16, 512, 2048], P('rep'), parts along dimension 0
- output 2: bfloat16 [16, 512, 2048], P('rep'), parts along dimension 0
- output 3: bfloat16 [16, 2048, 512], P('rep'), parts along dimension 0
- output 4: float32 [16, 512, 2048], P('rep'), parts along dimension 0
- output 5: float32 [16, 512, 2048], P('rep'), parts along dimension 0
- output 6: float32 [16, 2048, 512], P('rep'), parts along dimension 0
- output 7: float32 [16, 512, 2048], P('rep'), parts along dimension 0
- output 8: float32 [16, 512, 2048], P('rep'), parts along dimension 0
- output 9: float32 [16, 2048, 512], P('rep'), parts along dimension 0
There are 8 independent parts. The reference program is written for one: setup_inputs(seed, part) draws one part's arguments, and reference() takes and returns one part's arrays. A program takes and returns all parts, laid end to end along the dimension named above; an argument that names none is the same for every part.
All inputs are finite; a program needn't handle non-finite values.
Results may differ from the reference program's by a relative error of at most 0.02.
Values are sent between devices in bfloat16 or wider.
A program may use at most 768 MiB of HBM per device.

```python
import jax
import jax.numpy as jnp
from jax import lax

SEQUENCES = 8
TOKENS = 4096
D = 512
FF = 2048
LAYERS = 2
NAMES = ("w_gate", "w_up", "w_down")
SHAPES = {"w_gate": (LAYERS, D, FF), "w_up": (LAYERS, D, FF), "w_down": (LAYERS, FF, D)}


def bump(key, n, height):
    away = (jnp.arange(n, dtype=jnp.int32) - jax.random.randint(key, (), 0, n, jnp.int32)) % n
    return jnp.where(away < n // 8, height, 1.0)


def together(key, own, strength):
    shared = jax.random.normal(key, own.shape[1:], jnp.float32)
    return (own + strength * shared) * lax.rsqrt(1 + strength * strength)


def setup_inputs(seed: int = 0, part: int = 0) -> dict:
    kx, kdy, ka, kb, kz, kf, kh, kl, *keys = jax.random.split(jax.random.key(seed), 8 + 3 * len(NAMES))
    kx, kdy, ka, kb = (jax.random.fold_in(k, part) for k in (kx, kdy, ka, kb))
    kw, km, kv = (keys[i::3] for i in range(3))
    shape = (SEQUENCES, TOKENS, D)
    much_x, much_dy = jax.random.uniform(kz, (2,), jnp.float32, 0.0, 1.0)
    loud = 2.0 ** jax.random.uniform(jax.random.fold_in(kz, 1), (), jnp.float32, -1.0, 2.0)
    layers = 2.0 ** jax.random.uniform(kl, (LAYERS, 1, 1), jnp.float32, -1.0, 1.0)
    x = together(ka, jax.random.normal(kx, shape, jnp.float32), much_x) * bump(kf, D, 4.0)
    dy = together(kb, jax.random.normal(kdy, shape, jnp.float32), much_dy)
    drawn = {"x": x.astype(jnp.bfloat16), "dy": (loud * dy * (SEQUENCES * TOKENS) ** -0.5).astype(jnp.bfloat16)}
    for key, name in zip(kw, NAMES, strict=True):
        w = jax.random.normal(key, SHAPES[name], jnp.float32) * SHAPES[name][1] ** -0.5
        drawn[name] = (w * {"w_gate": 1.0, "w_up": bump(kh, FF, 4.0), "w_down": layers}[name]).astype(jnp.bfloat16)
    for key, name in zip(km, NAMES, strict=True):
        drawn[f"m_{name}"] = 0.1 * jax.random.normal(key, SHAPES[name], jnp.float32)
    for key, name in zip(kv, NAMES, strict=True):
        drawn[f"v_{name}"] = jax.random.uniform(key, SHAPES[name], jnp.float32, 0.005, 0.015)
    return drawn


def matmul(a, w):
    return jnp.dot(a, w, preferred_element_type=jnp.float32).astype(jnp.bfloat16)


def normed(h):
    wide = h.astype(jnp.float32)
    scale = lax.rsqrt(jnp.mean(wide**2, -1, keepdims=True) + 1e-6)
    return (wide * scale).astype(jnp.bfloat16)


def layer(h, w):
    a = normed(h)
    gate = jnp.dot(a, w["w_gate"], preferred_element_type=jnp.float32)
    up = jnp.dot(a, w["w_up"], preferred_element_type=jnp.float32)
    return h + matmul((jax.nn.silu(gate) * up).astype(jnp.bfloat16), w["w_down"])


def adamw(w, m, v, g):
    m = 0.9 * m + 0.1 * g
    v = 0.95 * v + 0.05 * g * g
    step = m * lax.rsqrt(v + 1e-8) + 0.1 * w
    return (w - 0.02 * step).astype(jnp.bfloat16), m, v


def stack(weights, h):
    return lax.scan(lambda h, w: (layer(h, w), None), h, weights)[0]


def reference(x, dy, w_gate, w_up, w_down, m_w_gate, m_w_up, m_w_down, v_w_gate, v_w_up, v_w_down):
    weights = dict(zip(NAMES, (w_gate, w_up, w_down), strict=True))

    def take(so_far, sequence):
        h, by_y = sequence
        _, back = jax.vjp(lambda w: stack(w, h), weights)
        return jax.tree.map(lambda total, term: total + term.astype(jnp.float32), so_far, back(by_y)[0]), None

    none_yet = {name: jnp.zeros(w.shape, jnp.float32) for name, w in weights.items()}
    by_weights, _ = lax.scan(take, none_yet, (x, dy))
    gradients = [by_weights[name].astype(jnp.bfloat16).astype(jnp.float32) for name in NAMES]
    new = [
        adamw(w.astype(jnp.float32), m, v, g)
        for w, m, v, g in zip((w_gate, w_up, w_down), (m_w_gate, m_w_up, m_w_down), (v_w_gate, v_w_up, v_w_down), gradients, strict=True)
    ]
    return tuple(one[which] for which in range(3) for one in new)
```

```python
import functools

import jax
import jax.numpy as jnp
from jax import lax
from jax.experimental import pallas as pl
from jax.experimental.pallas import tpu as pltpu
from jax.sharding import PartitionSpec as P

F32, BF16 = jnp.float32, jnp.bfloat16
FB = 256
FTM = 512
TM = 1024
VMEM_LIMIT = 64 * 1024 * 1024 - 64 * 1024


def dot(a, b):
    return jnp.dot(a, b, preferred_element_type=F32)


def dot_nt(a, b):
    return lax.dot_general(a, b, (((1,), (1,)), ((), ())), preferred_element_type=F32)


def scale_of(wide):
    return lax.rsqrt(jnp.mean(wide * wide, -1, keepdims=True) + 1e-6)


def normed(h):
    wide = h.astype(F32)
    return (wide * scale_of(wide)).astype(BF16)


def sigmoid(x):
    return 1.0 / (1.0 + jnp.exp(-x))


def at(index, size):
    return pl.ds(pl.multiple_of(index * size, size), size)


def fetch(layer, sources, refs, sem):
    copies = [pltpu.make_async_copy(source.at[layer], ref, sem.at[k]) for k, (source, ref) in enumerate(zip(sources, refs, strict=True))]
    for copy in copies:
        copy.start()
    return copies


def forward_kernel(x_ref, wg_all, wu_all, wd_all, h_ref, wg_ref, wu_ref, wd_ref, sem, prod_ref):
    tokens, ff = x_ref.shape[0], wg_ref.shape[1]
    for copy in fetch(0, (wg_all, wu_all, wd_all), (wg_ref, wu_ref, wd_ref), sem):
        copy.wait()

    def tile(i, _):
        rows = at(i, FTM)
        x = x_ref[rows, :]
        a = normed(x)
        for c in range(0, ff, 512):
            gate = dot(a, wg_ref[:, c : c + 512])
            up = dot(a, wu_ref[:, c : c + 512])
            prod_ref[:, c : c + 512] = (gate * sigmoid(gate) * up).astype(BF16)
        y = dot(prod_ref[...], wd_ref[...]).astype(BF16)
        h_ref[rows, :] = (x.astype(F32) + y.astype(F32)).astype(BF16)
        return _

    lax.fori_loop(0, tokens // FTM, tile, 0)


def grads_loop(a_ref, at_ref, d_ref, dt_ref, wg_ref, wu_ref, wd_ref, da_ref, g_ref, prod_ref, dgate_ref, dup_ref, acc_ref):
    tokens, ff = a_ref.shape[0], wg_ref.shape[1]
    tiles = tokens // TM
    steps = (ff // FB) * tiles

    def first(t):
        j, i, slot = t // tiles, t % tiles, t % 2
        rows, cols = at(i, TM), at(j, FB)
        a, d = a_ref[rows, :], d_ref[rows, :]
        gate = dot(a, wg_ref[:, cols])
        up = dot(a, wu_ref[:, cols])
        dprod = dot_nt(d, wd_ref[cols, :]).astype(BF16).astype(F32)
        sig = sigmoid(gate)
        silu = gate * sig
        prod_ref[slot] = (silu * up).astype(BF16)
        dup_ref[slot] = (dprod * silu).astype(BF16)
        dgate_ref[slot] = (dprod * up * (sig * (1.0 + gate * (1.0 - sig)))).astype(BF16)

    def second(t):
        j, i, slot = t // tiles, t % tiles, t % 2
        rows, cols = at(i, TM), at(j, FB)
        fresh = i == 0
        dt, a_t = dt_ref[:, rows], at_ref[:, rows]
        prod, dgate, dup = prod_ref[slot], dgate_ref[slot], dup_ref[slot]
        for k, (left, right) in enumerate(((dt, prod), (a_t, dgate), (a_t, dup))):
            acc_ref[k] = jnp.where(fresh, 0.0, acc_ref[k]) + dot(left, right)
        if da_ref is not None:
            da = dot_nt(dgate, wg_ref[:, cols]) + dot_nt(dup, wu_ref[:, cols])
            da_ref[rows, :] = jnp.where(j == 0, 0.0, da_ref[rows, :]) + da

        @pl.when(i == tiles - 1)
        def _():
            d = g_ref.shape[2]
            for n in range(0, acc_ref.shape[1], d):
                g_ref[j, n : n + d, :] = acc_ref[0, n : n + d, :].T.astype(BF16)
            half = acc_ref.shape[1]
            g_ref[j, half : 2 * half, :] = acc_ref[1].astype(BF16)
            g_ref[j, 2 * half :, :] = acc_ref[2].astype(BF16)

    first(0)

    def step(t, _):
        first(t)
        second(t - 1)
        return _

    lax.fori_loop(1, steps, step, 0)
    second(steps - 1)


def last_layer_kernel(h_ref, dy_ref, wg_all, wu_all, wd_all, da_ref, g_ref, wg_ref, wu_ref, wd_ref, sem, a_ref, at_ref, dt_ref, *scratch):
    copies = fetch(1, (wg_all, wu_all, wd_all), (wg_ref, wu_ref, wd_ref), sem)

    def tile(i, _):
        rows = at(i, FTM)
        a = normed(h_ref[rows, :])
        a_ref[rows, :] = a
        at_ref[:, rows] = a.T
        dt_ref[:, rows] = dy_ref[rows, :].T
        return _

    lax.fori_loop(0, h_ref.shape[0] // FTM, tile, 0)
    for copy in copies:
        copy.wait()
    grads_loop(a_ref, at_ref, dy_ref, dt_ref, wg_ref, wu_ref, wd_ref, da_ref, g_ref, *scratch)


def first_layer_kernel(x_ref, h_ref, dy_ref, da_ref, wg_all, wu_all, wd_all, g_ref, wg_ref, wu_ref, wd_ref, sem, a_ref, at_ref, d_ref, dt_ref, *scratch):
    copies = fetch(0, (wg_all, wu_all, wd_all), (wg_ref, wu_ref, wd_ref), sem)

    def tile(i, _):
        rows = at(i, FTM)
        a = normed(x_ref[rows, :])
        a_ref[rows, :] = a
        at_ref[:, rows] = a.T
        wide = h_ref[rows, :].astype(F32)
        scale = scale_of(wide)
        da = da_ref[rows, :].astype(BF16).astype(F32)
        inner = jnp.mean(da * wide, -1, keepdims=True)
        dh = (scale * da - wide * (scale * scale * scale * inner)).astype(BF16)
        d = (dy_ref[rows, :].astype(F32) + dh.astype(F32)).astype(BF16)
        d_ref[rows, :] = d
        dt_ref[:, rows] = d.T
        return _

    lax.fori_loop(0, x_ref.shape[0] // FTM, tile, 0)
    for copy in copies:
        copy.wait()
    grads_loop(a_ref, at_ref, d_ref, dt_ref, wg_ref, wu_ref, wd_ref, None, g_ref, *scratch)


def grads_scratch(d):
    return [
        pltpu.VMEM((2, TM, FB), BF16),
        pltpu.VMEM((2, TM, FB), BF16),
        pltpu.VMEM((2, TM, FB), BF16),
        pltpu.VMEM((3, d, FB), F32),
    ]


def adam_kernel(g_ref, *refs):
    ins, outs = refs[:9], refs[-9:]
    d = ins[0].shape[0]
    fb = g_ref.shape[1]
    for k in range(3):
        w_ref, m_ref, v_ref = ins[k], ins[3 + k], ins[6 + k]
        ow, om, ov = outs[k], outs[3 + k], outs[6 + k]
        if k < 2:
            pieces = [((slice(None), slice(None)), slice(d + k * d, d + (k + 1) * d))]
        else:
            pieces = [((slice(None), slice(n, n + fb)), slice(n, n + fb)) for n in range(0, d, fb)]
        for place, rows in pieces:
            g = g_ref[rows, :].astype(F32)
            m = 0.9 * m_ref[place] + 0.1 * g
            v = 0.95 * v_ref[place] + 0.05 * g * g
            w = w_ref[place].astype(F32)
            ow[place] = (w - 0.02 * (m * lax.rsqrt(v + 1e-8) + 0.1 * w)).astype(BF16)
            om[place] = m
            ov[place] = v


def adam(layer, g, weights, moments, into):
    layers, d, ff = weights[0].shape
    wide = pl.BlockSpec((None, d, FB), lambda j: (layer, 0, j))
    tall = pl.BlockSpec((None, FB, d), lambda j: (layer, j, 0))
    specs = [wide, wide, tall] * 3
    arrays = [*weights, *moments]
    out_shape = [jax.ShapeDtypeStruct(a.shape, a.dtype) for a in arrays]
    extra = [] if into is None else list(into)
    return pl.pallas_call(
        adam_kernel,
        grid=(ff // FB,),
        out_shape=out_shape,
        in_specs=[pl.BlockSpec((None, *g.shape[1:]), lambda j: (j, 0, 0)), *specs, *[pl.BlockSpec(memory_space=pl.ANY)] * len(extra)],
        out_specs=specs,
        input_output_aliases={10 + k: k for k in range(len(extra))},
        cost_estimate=pl.CostEstimate(flops=60 * d * ff, bytes_accessed=3 * 22 * d * ff, transcendentals=3 * d * ff),
        compiler_params=pltpu.CompilerParams(vmem_limit_bytes=40 * 1024 * 1024),
        name="adam",
    )(g, *arrays, *extra)


def solution(mesh):
    def step(x, dy, *arrays):
        weights, moments = arrays[:3], arrays[3:]
        layers, d, ff = weights[0].shape
        x, dy = x[0], dy[0]
        tokens = x.shape[0]
        blocks = ff // FB
        whole = pl.BlockSpec(memory_space=pltpu.VMEM)

        any3 = [pl.BlockSpec(memory_space=pl.ANY)] * 3
        held = [pltpu.VMEM((d, ff), BF16), pltpu.VMEM((d, ff), BF16), pltpu.VMEM((ff, d), BF16), pltpu.SemaphoreType.DMA((3,))]

        params = pltpu.CompilerParams(vmem_limit_bytes=VMEM_LIMIT)
        flops = 2 * tokens * d * ff
        g_shape = jax.ShapeDtypeStruct((blocks, 3 * d, FB), BF16)
        h = pl.pallas_call(
            forward_kernel,
            out_shape=jax.ShapeDtypeStruct((tokens, d), BF16),
            in_specs=[whole, *any3],
            out_specs=whole,
            scratch_shapes=[*held, pltpu.VMEM((FTM, ff), BF16)],
            cost_estimate=pl.CostEstimate(flops=3 * flops, bytes_accessed=0, transcendentals=0),
            compiler_params=params,
            name="forward",
        )(x, *weights)
        da, g1 = pl.pallas_call(
            last_layer_kernel,
            out_shape=[jax.ShapeDtypeStruct((tokens, d), F32), g_shape],
            in_specs=[whole, whole, *any3],
            out_specs=[whole, whole],
            scratch_shapes=[*held, pltpu.VMEM((tokens, d), BF16), pltpu.VMEM((d, tokens), BF16), pltpu.VMEM((d, tokens), BF16), *grads_scratch(d)],
            cost_estimate=pl.CostEstimate(flops=8 * flops, bytes_accessed=0, transcendentals=0),
            compiler_params=params,
            name="last_layer",
        )(h, dy, *weights)
        s1 = lax.psum(g1, "dp")
        g0 = pl.pallas_call(
            first_layer_kernel,
            out_shape=g_shape,
            in_specs=[whole] * 4 + any3,
            out_specs=whole,
            scratch_shapes=[
                *held,
                pltpu.VMEM((tokens, d), BF16),
                pltpu.VMEM((d, tokens), BF16),
                pltpu.VMEM((tokens, d), BF16),
                pltpu.VMEM((d, tokens), BF16),
                *grads_scratch(d),
            ],
            cost_estimate=pl.CostEstimate(flops=6 * flops, bytes_accessed=0, transcendentals=0),
            compiler_params=params,
            name="first_layer",
        )(x, h, dy, da, *weights)
        g0, s1 = lax.optimization_barrier((g0, s1))
        s0 = lax.psum(g0, "dp")
        new = adam(1, s1, weights, moments, None)
        return tuple(adam(0, s0, weights, moments, new))

    return jax.shard_map(
        step,
        mesh=mesh,
        in_specs=(P(("rep", "dp"), None, None),) * 2 + (P(None, None, None),) * 9,
        out_specs=(P("rep", None, None),) * 9,
        check_vma=False,
    )
```

```python
import functools

import jax
import jax.numpy as jnp
from jax import lax
from jax.experimental import pallas as pl
from jax.experimental.pallas import tpu as pltpu
from jax.sharding import PartitionSpec as P

F32, BF16 = jnp.float32, jnp.bfloat16
MESH = pl.DeviceIdType.MESH
SB = 128
FB = 2 * SB
FTM = 512
TM = 1024
VMEM_LIMIT = 64 * 1024 * 1024 - 64 * 1024


def dot(a, b):
    return jnp.dot(a, b, preferred_element_type=F32)


def dot_nt(a, b):
    return lax.dot_general(a, b, (((1,), (1,)), ((), ())), preferred_element_type=F32)


def scale_of(wide):
    return lax.rsqrt(jnp.mean(wide * wide, -1, keepdims=True) + 1e-6)


def normed(h):
    wide = h.astype(F32)
    return (wide * scale_of(wide)).astype(BF16)


def sigmoid(x):
    return 1.0 / (1.0 + jnp.exp(-x))


def at(index, size):
    return pl.ds(pl.multiple_of(index * size, size), size)


def forward_kernel(x_ref, wg_all, wu_all, wd_all, h_ref, wg_ref, wu_ref, wd_ref, sem, prod_ref):
    tokens, ff = x_ref.shape[0], wg_ref.shape[1]
    copies = [
        pltpu.make_async_copy(source.at[0], ref, sem.at[k])
        for k, (source, ref) in enumerate(((wg_all, wg_ref), (wu_all, wu_ref), (wd_all, wd_ref)))
    ]
    for copy in copies:
        copy.start()
    for copy in copies:
        copy.wait()

    def tile(i, _):
        rows = at(i, FTM)
        x = x_ref[rows, :]
        a = normed(x)
        for c in range(0, ff, 512):
            gate = dot(a, wg_ref[:, c : c + 512])
            up = dot(a, wu_ref[:, c : c + 512])
            prod_ref[:, c : c + 512] = (gate * sigmoid(gate) * up).astype(BF16)
        y = dot(prod_ref[...], wd_ref[...]).astype(BF16)
        h_ref[rows, :] = (x.astype(F32) + y.astype(F32)).astype(BF16)
        return _

    lax.fori_loop(0, tokens // FTM, tile, 0)


def backward_kernel(
    n,
    x_hbm,
    h_hbm,
    dy_hbm,
    wg_hbm,
    wu_hbm,
    wd_hbm,
    g1_hbm,
    g0a_hbm,
    g0b_hbm,
    a_ref,
    at_ref,
    d_ref,
    dt_ref,
    da_ref,
    prod_ref,
    dgate_ref,
    dup_ref,
    acc_ref,
    wg_ref,
    wu_ref,
    wd_ref,
    own_ref,
    recv_ref,
    xs_ref,
    hs_ref,
    in_sem,
    w_sem,
    s_sem,
    send_sem,
    recv_sem,
    ag_send_sem,
    ag_recv_sem,
    out_sem,
):
    me = lax.axis_index("dp")
    right, left = lax.rem(me + 1, n), lax.rem(me + n - 1, n)
    tokens, d = a_ref.shape
    tiles = tokens // TM
    half = n // 2
    blocks = 2 * half
    steps = blocks * tiles
    spans = tokens // FTM
    halves = (slice(0, d // 2), slice(d // 2, d))
    sides = (right, left)

    def around(k):
        return lax.rem(me + k + 2 * n, n)

    def rs_copy(par, side, stage, pos):
        if isinstance(stage, int) and stage == 0:
            src = own_ref.at[par, pos, :, halves[side], :]
            dst = recv_ref.at[par, side, 0, :, halves[side], :]
        else:
            src = own_ref.at[par, pos]
            dst = recv_ref.at[par, side, stage]
        return pltpu.make_async_remote_copy(
            src, dst, send_sem.at[par, side, stage], recv_sem.at[par, side, stage], device_id={"dp": sides[side]}, device_id_type=MESH
        )

    def ag_copy(p, side, hop):
        owner = around(-hop if side == 0 else hop)
        place = g1_hbm.at[owner, p]
        if hop == half - 1:
            place = g1_hbm.at[owner, p, :, halves[side], :]
        src = own_ref.at[p, blocks - 1] if hop == 0 else place
        return pltpu.make_async_remote_copy(
            src, place, ag_send_sem.at[p, side, hop], ag_recv_sem.at[p, side, hop], device_id={"dp": sides[side]}, device_id_type=MESH
        )

    def first_stage(par):
        for side in range(2):
            rs_copy(par, side, 0, 0).start()

    def next_stage(par, side, stage, pos):
        @pl.when(stage == 1)
        def _():
            rs_copy(par, side, 0, 0).wait_recv()
            rows = halves[side]
            own_ref[par, pos, :, rows, :] = (
                own_ref[par, pos, :, rows, :].astype(F32) + recv_ref[par, side, 0, :, rows, :].astype(F32)
            ).astype(BF16)

        @pl.when(stage > 1)
        def _():
            rs_copy(par, side, stage - 1, pos).wait_recv()
            own_ref[par, pos] = (own_ref[par, pos].astype(F32) + recv_ref[par, side, stage - 1].astype(F32)).astype(BF16)

        rs_copy(par, side, stage, pos).start()

    def last_stage(par):
        for side in range(2):
            rs_copy(par, side, half - 1, 0).wait_recv()
        total = own_ref[par, blocks - 1].astype(F32)
        for side in range(2):
            total = total + recv_ref[par, side, half - 1].astype(F32)
        own_ref[par, blocks - 1] = total.astype(BF16)
        for side in range(2):
            for stage in range(half):
                rs_copy(par, side, stage, 0).wait_send()

    def ag_hop(p, hop):
        for side in range(2):
            if hop > 0:
                ag_copy(p, side, hop - 1).wait_recv()
            if hop < half:
                ag_copy(p, side, hop).start()
        for side in range(2):
            if hop > 0:
                ag_copy(p, side, hop - 1).wait_send()

    def ag_first(p):
        ag_hop(p, 0)
        pltpu.make_async_copy(own_ref.at[p, blocks - 1], g1_hbm.at[me, p], out_sem.at[p]).start()

    def ag_own_done(p):
        pltpu.make_async_copy(own_ref.at[p, blocks - 1], g1_hbm.at[me, p], out_sem.at[p]).wait()

    def weight_copies(layer, b):
        p, q, slot = b // half, b % half, b % 2
        copies = []
        for k, owner in enumerate((around(q + half), around(half - 1 - q))):
            cols = pl.ds(pl.multiple_of(owner * FB + p * SB, SB), SB)
            place = slice(k * SB, (k + 1) * SB)
            copies += [
                pltpu.make_async_copy(wg_hbm.at[layer, :, cols], wg_ref.at[slot, :, place], w_sem.at[slot, 3 * k]),
                pltpu.make_async_copy(wu_hbm.at[layer, :, cols], wu_ref.at[slot, :, place], w_sem.at[slot, 3 * k + 1]),
                pltpu.make_async_copy(wd_hbm.at[layer, cols, :], wd_ref.at[slot, place, :], w_sem.at[slot, 3 * k + 2]),
            ]
        return copies

    def fetch(layer, b):
        for copy in weight_copies(layer, b):
            copy.start()

    def fetched(layer, b):
        for copy in weight_copies(layer, b):
            copy.wait()

    def first(t):
        b, i, slot = t // tiles, t % tiles, t % 2
        rows, ws = at(i, TM), b % 2
        a, dd = a_ref[rows, :], d_ref[rows, :]
        gate = dot(a, wg_ref[ws])
        up = dot(a, wu_ref[ws])
        dprod = dot_nt(dd, wd_ref[ws]).astype(BF16).astype(F32)
        sig = sigmoid(gate)
        silu = gate * sig
        prod_ref[slot] = (silu * up).astype(BF16)
        dup_ref[slot] = (dprod * silu).astype(BF16)
        dgate_ref[slot] = (dprod * up * (sig * (1.0 + gate * (1.0 - sig)))).astype(BF16)

    def second(t, with_da):
        b, i, slot = t // tiles, t % tiles, t % 2
        rows, ws = at(i, TM), b % 2
        fresh = i == 0
        dt, a_t = dt_ref[:, rows], at_ref[:, rows]
        prod, dgate, dup = prod_ref[slot], dgate_ref[slot], dup_ref[slot]
        for k, (lhs, rhs) in enumerate(((a_t, dgate), (a_t, dup), (dt, prod))):
            acc_ref[k] = jnp.where(fresh, 0.0, acc_ref[k]) + dot(lhs, rhs)
        if with_da:
            da = dot_nt(dgate, wg_ref[ws]) + dot_nt(dup, wu_ref[ws])
            da_ref[rows, :] = jnp.where(b == 0, 0.0, da_ref[rows, :]) + da

        @pl.when(i == tiles - 1)
        def _():
            par, q = b // half, b % half
            for k in range(2):
                own_ref[par, 2 * q + k] = acc_ref[:, :, k * SB : (k + 1) * SB].astype(BF16)

    def middle(layer, b):
        p, q = b // half, b % half

        @pl.when(q > 0)
        def _():
            next_stage(p, 0, q, 2 * q - 1)

        if layer == 1:

            @pl.when(b == half)
            def _():
                last_stage(0)
                ag_first(0)

            for hop in range(1, half):

                @pl.when(b == half + hop)
                def _(hop=hop):
                    ag_hop(0, hop)

        else:

            @pl.when(b == 0)
            def _():
                last_stage(1)
                ag_first(1)

            @pl.when(b == 1)
            def _():
                ag_hop(0, half)
                ag_own_done(0)

            for hop in range(1, half):

                @pl.when(b == 2 * hop)
                def _(hop=hop):
                    ag_hop(1, hop)
                    if hop == 1:
                        ag_own_done(1)

            @pl.when(b == half)
            def _():
                last_stage(0)
                pltpu.make_async_copy(own_ref.at[0, blocks - 1], g0a_hbm, out_sem.at[0]).start()

    def end(layer, b):
        p, q = b // half, b % half

        @pl.when(q == 0)
        def _():
            first_stage(p)

        @pl.when(q > 0)
        def _():
            next_stage(p, 1, q, 2 * q)

    def layer_loop(layer):
        with_da = layer == 1
        fetched(layer, 0)
        fetch(layer, 1)
        first(0)

        def step(t, _):
            @pl.when(t % tiles == 0)
            def _():
                fetched(layer, t // tiles)

            @pl.when((t % tiles == 1) & (t > tiles) & (t < steps - tiles))
            def _():
                fetch(layer, t // tiles + 1)

            first(t)
            second(t - 1, with_da)
            b, i = (t - 1) // tiles, (t - 1) % tiles

            @pl.when(i == tiles // 2 - 1)
            def _():
                middle(layer, b)

            @pl.when(i == tiles - 1)
            def _():
                end(layer, b)

            return 0

        lax.fori_loop(1, steps, step, 0)
        if layer == 1:
            fetch(0, 0)
        second(steps - 1, with_da)
        end(layer, blocks - 1)

    barrier = pltpu.get_barrier_semaphore()
    for side in sides:
        pl.semaphore_signal(barrier, inc=1, device_id={"dp": side}, device_id_type=MESH)

    def load(i, k):
        rows = at(i, FTM)
        return pltpu.make_async_copy((h_hbm, dy_hbm)[k].at[rows, :], (a_ref, d_ref)[k].at[rows, :], in_sem.at[k, i])

    fetch(1, 0)
    for i in range(spans):
        for k in range(2):
            load(i, k).start()

    def prepare(i, _):
        rows = at(i, FTM)
        load(i, 0).wait()
        load(i, 1).wait()
        a = normed(a_ref[rows, :])
        a_ref[rows, :] = a
        at_ref[:, rows] = a.T
        dt_ref[:, rows] = d_ref[rows, :].T
        return 0

    lax.fori_loop(0, spans, prepare, 0)
    pl.semaphore_wait(barrier, 2)

    def restage(i, k):
        return pltpu.make_async_copy((x_hbm, h_hbm)[k].at[at(i, FTM), :], (xs_ref, hs_ref)[k].at[i % 2], s_sem.at[k, i % 2])

    for i in range(2):
        for k in range(2):
            restage(i, k).start()
    layer_loop(1)

    def between(i, _):
        rows = at(i, FTM)
        for k in range(2):
            restage(i, k).wait()
        a = normed(xs_ref[i % 2])
        a_ref[rows, :] = a
        at_ref[:, rows] = a.T
        wide = hs_ref[i % 2].astype(F32)
        scale = scale_of(wide)
        da = da_ref[rows, :].astype(BF16).astype(F32)
        inner = jnp.mean(da * wide, -1, keepdims=True)
        dh = (scale * da - wide * (scale * scale * scale * inner)).astype(BF16)
        dd = (d_ref[rows, :].astype(F32) + dh.astype(F32)).astype(BF16)
        d_ref[rows, :] = dd
        dt_ref[:, rows] = dd.T

        @pl.when(i < spans - 2)
        def _():
            for k in range(2):
                restage(i + 2, k).start()

        return 0

    lax.fori_loop(0, spans, between, 0)
    layer_loop(0)
    last_stage(1)
    out = pltpu.make_async_copy(own_ref.at[1, blocks - 1], g0b_hbm, out_sem.at[2])
    out.start()
    ag_hop(1, half)
    pltpu.make_async_copy(own_ref.at[0, blocks - 1], g0a_hbm, out_sem.at[0]).wait()
    out.wait()


def adam_kernel(count, *refs):
    gs, ins, outs = refs[:count], refs[count : count + 9], refs[-9:]
    for h, g_ref in enumerate(gs):
        here = slice(h * SB, (h + 1) * SB)
        for k in range(3):
            g = g_ref[k].astype(F32)
            place = (slice(None), here)
            if k == 2:
                g = g.T
                place = (here, slice(None))
            w_ref, m_ref, v_ref = ins[k], ins[3 + k], ins[6 + k]
            ow, om, ov = outs[k], outs[3 + k], outs[6 + k]
            m = 0.9 * m_ref[place] + 0.1 * g
            v = 0.95 * v_ref[place] + 0.05 * g * g
            w = w_ref[place].astype(F32)
            ow[place] = (w - 0.02 * (m * lax.rsqrt(v + 1e-8) + 0.1 * w)).astype(BF16)
            om[place] = m
            ov[place] = v


def adam_all_kernel(g_ref, *refs):
    adam_kernel(2, g_ref.at[0], g_ref.at[1], *refs)


def adam_specs(layer, d, owner):
    wide = pl.BlockSpec((None, d, FB), lambda j, *s: (layer, 0, owner(j, *s)))
    tall = pl.BlockSpec((None, FB, d), lambda j, *s: (layer, owner(j, *s), 0))
    return [wide, wide, tall] * 3


ANY = pl.BlockSpec(memory_space=pl.ANY)


def estimate(d, blocks):
    return pl.CostEstimate(flops=3_000_000_000 * blocks, bytes_accessed=3 * 22 * d * FB * blocks, transcendentals=0)


def adam_all(layer, g, arrays, start, count, into):
    d = arrays[0].shape[1]
    specs = adam_specs(layer, d, lambda j: j + start)
    extra = [] if into is None else list(into)
    return pl.pallas_call(
        adam_all_kernel,
        grid=(count,),
        out_shape=[jax.ShapeDtypeStruct(a.shape, a.dtype) for a in arrays],
        in_specs=[pl.BlockSpec((None, *g.shape[1:]), lambda j: (j + start, 0, 0, 0, 0)), *specs, *[ANY] * len(extra)],
        out_specs=specs,
        input_output_aliases={10 + k: k for k in range(len(extra))},
        cost_estimate=estimate(d, count),
        compiler_params=pltpu.CompilerParams(vmem_limit_bytes=VMEM_LIMIT),
        name=f"adam_last_{start}",
    )(g, *arrays, *extra)


def adam_owner_kernel(pairs, owners, *refs):
    gs, refs = refs[: 2 * pairs], refs[2 * pairs :]
    refs = [*refs[:9], *refs[18:]]
    for k in range(pairs):

        @pl.when(pl.program_id(0) == k)
        def _(k=k):
            adam_kernel(2, *gs[2 * k : 2 * k + 2], *refs)


def adam_owners(layer, pairs, owners, arrays, into):
    d = arrays[0].shape[1]
    specs = adam_specs(layer, d, lambda j, owners: owners[j])
    gs = [g for pair in pairs for g in pair]
    whole = pl.BlockSpec(gs[0].shape, lambda j, owners: (0, 0, 0))
    count = len(pairs)
    return pl.pallas_call(
        functools.partial(adam_owner_kernel, count),
        grid_spec=pltpu.PrefetchScalarGridSpec(
            num_scalar_prefetch=1, grid=(count,), in_specs=[*[whole] * len(gs), *specs, *[ANY] * 9], out_specs=specs
        ),
        out_shape=[jax.ShapeDtypeStruct(a.shape, a.dtype) for a in arrays],
        input_output_aliases={1 + len(gs) + 9 + k: k for k in range(9)},
        cost_estimate=estimate(d, count),
        compiler_params=pltpu.CompilerParams(vmem_limit_bytes=VMEM_LIMIT),
        name="adam_first",
    )(jnp.stack(owners).astype(jnp.int32), *gs, *arrays, *into)


def solution(mesh):
    n = mesh.shape["dp"]

    def step(x, dy, *arrays):
        weights = arrays[:3]
        _, d, ff = weights[0].shape
        x, dy = x[0], dy[0]
        tokens = x.shape[0]
        half = n // 2
        whole = pl.BlockSpec(memory_space=pltpu.VMEM)
        flops = 2 * tokens * d * ff
        h = pl.pallas_call(
            forward_kernel,
            out_shape=jax.ShapeDtypeStruct((tokens, d), BF16),
            in_specs=[whole, ANY, ANY, ANY],
            out_specs=whole,
            scratch_shapes=[
                pltpu.VMEM((d, ff), BF16),
                pltpu.VMEM((d, ff), BF16),
                pltpu.VMEM((ff, d), BF16),
                pltpu.SemaphoreType.DMA((3,)),
                pltpu.VMEM((FTM, ff), BF16),
            ],
            cost_estimate=pl.CostEstimate(flops=3 * flops, bytes_accessed=0, transcendentals=0),
            compiler_params=pltpu.CompilerParams(vmem_limit_bytes=VMEM_LIMIT),
            name="forward",
        )(x, *weights)
        shard = (3, d, SB)
        dma = pltpu.SemaphoreType.DMA
        g1, g0a, g0b = pl.pallas_call(
            functools.partial(backward_kernel, n),
            out_shape=[jax.ShapeDtypeStruct((n, 2, *shard), BF16), *[jax.ShapeDtypeStruct(shard, BF16)] * 2],
            in_specs=[ANY] * 6,
            out_specs=[ANY] * 3,
            scratch_shapes=[
                pltpu.VMEM((tokens, d), BF16),
                pltpu.VMEM((d, tokens), BF16),
                pltpu.VMEM((tokens, d), BF16),
                pltpu.VMEM((d, tokens), BF16),
                pltpu.VMEM((tokens, d), F32),
                pltpu.VMEM((2, TM, FB), BF16),
                pltpu.VMEM((2, TM, FB), BF16),
                pltpu.VMEM((2, TM, FB), BF16),
                pltpu.VMEM((3, d, FB), F32),
                pltpu.VMEM((2, d, FB), BF16),
                pltpu.VMEM((2, d, FB), BF16),
                pltpu.VMEM((2, FB, d), BF16),
                pltpu.VMEM((2, n, *shard), BF16),
                pltpu.VMEM((2, 2, half, *shard), BF16),
                pltpu.VMEM((2, FTM, d), BF16),
                pltpu.VMEM((2, FTM, d), BF16),
                dma((2, tokens // FTM)),
                dma((2, 6)),
                dma((2, 2)),
                dma((2, 2, half)),
                dma((2, 2, half)),
                dma((2, 2, half)),
                dma((2, 2, half)),
                dma((3,)),
            ],
            cost_estimate=pl.CostEstimate(flops=14 * flops, bytes_accessed=0, transcendentals=0),
            compiler_params=pltpu.CompilerParams(collective_id=0, has_side_effects=True, vmem_limit_bytes=VMEM_LIMIT),
            name="backward",
        )(x, h, dy, *weights)

        me = lax.axis_index("dp")
        turns = [[(i, (i + 1) % n) for i in range(n)], [(i, (i - 1) % n) for i in range(n)]]
        hops, now = [], [[g0a, g0b], [g0a, g0b]]
        for hop in range(1, half):
            now = [[lax.ppermute(g, "dp", turns[side]) for g in now[side]] for side in range(2)]
            hops.append(now)
        opposite = [lax.ppermute(now[side][side], "dp", turns[side]) for side in range(2)]

        new = adam_all(1, g1, arrays, 0, half, None)
        new = adam_all(1, g1, arrays, half, half, new)
        new = adam_owners(0, [[g0a, g0b]], [me], arrays, new)
        for hop, pairs in enumerate(hops, 1):
            new = adam_owners(0, pairs, [(me + n - hop) % n, (me + hop) % n], arrays, new)
        return tuple(adam_owners(0, [opposite], [(me + half) % n], arrays, new))

    return jax.shard_map(
        step,
        mesh=mesh,
        in_specs=(P(("rep", "dp"), None, None),) * 2 + (P(None, None, None),) * 9,
        out_specs=(P("rep", None, None),) * 9,
        check_vma=False,
    )
```
